32 devices in a mesh: row: 4 (over y, x), col: 8 (over z, core).
Axes of the slice: x: 2, y: 2, z: 4, core: 2. Of those that a mesh axis runs over, the one named last changes fastest.
Arguments:
- factors: float32 [1, 8192, 8192], P(None, 'row', 'col'), may hold values from -20 to 30, as said below
Outputs:
- refreshed: float32 [1, 8192, 8192], P(None, 'row', 'col')
The draws below stay inside these ranges and needn't reach their ends.
Inputs may be any that keep to these rules, and one draw needn't show every extreme that they name: `factors`: every factor is symmetric positive definite.
All inputs are finite; a program needn't handle non-finite values.
Results may differ from the reference program's by a relative error of at most 0.0003.
Values sent between devices are 32-bit elements; how exact they have to be, the bound alone decides.
No kernel may reach another device: no remote copies, remote signals or barrier semaphores. Data moves between devices by JAX's collectives and lax.ppermute only.
A program may use at most 64 MiB of HBM per device.

```python
import jax
import jax.numpy as jnp
from jax import lax

N = 8192
P_SIZE = 512
STEPS = 2
FACTORS = 1
N_COL = 8


def draw_factors(key, part):
    base_key = jax.random.fold_in(key, 11)
    position = jnp.arange(N, dtype=jnp.float32)
    rising = 3.0 ** (0.5 * position / N)
    scale_low, scale_high = (0.25, 0.75)

    def one_factor(member):
        noise_key, level_key, scale_key, shared_key = jax.random.split(jax.random.fold_in(base_key, member), 4)
        jitter = jax.random.normal(noise_key, (N, N), jnp.float32)
        shared = 0.5 * jax.random.truncated_normal(shared_key, -2.0, 2.0, (N, 8), jnp.float32)
        symmetric = (jitter + jitter.T) * (0.5 / jnp.sqrt(2.0 * N))
        common_part = jnp.dot(shared, shared.T, precision=lax.Precision.HIGHEST)
        levels = jax.random.uniform(level_key, (N,), jnp.float32, 2.0, 4.0)
        scales = jnp.exp(jax.random.uniform(scale_key, (N,), jnp.float32, jnp.log(scale_low), jnp.log(scale_high))) * rising
        matrix_core = symmetric + common_part + jnp.diag(levels)
        return scales[:, None] * matrix_core * scales[None, :]
    return lax.map(one_factor, jnp.arange(FACTORS))


def setup_inputs(seed: int = 0) -> dict:
    arg_keys = jax.random.split(jax.random.key(seed), 2)
    factors = draw_factors(jax.random.fold_in(arg_keys[1], 71), 0)
    return dict(factors=factors)


damping_share = 0.03162277660168379

def reference(factors):
    col_block = N // N_COL
    panel_slab = P_SIZE // N_COL
    sequence = jnp.arange(N, dtype=jnp.int32).reshape(N // col_block, col_block // panel_slab, panel_slab)
    sequence = sequence.transpose(1, 0, 2).reshape(N)
    restore = jnp.zeros((N,), jnp.int32).at[sequence].set(jnp.arange(N, dtype=jnp.int32))
    results = []
    for member in range(FACTORS):
        matrix = factors[member]
        damping = damping_share * jnp.trace(matrix) / N
        matrix = matrix + damping * jnp.eye(N, dtype=matrix.dtype)
        matrix = matrix[sequence][:, sequence]
        for section_no in range(STEPS):
            begin_at = section_no * P_SIZE
            finish = begin_at + P_SIZE
            factor_kk = jnp.linalg.cholesky(matrix[begin_at:finish, begin_at:finish])
            inverse_kk = jax.scipy.linalg.solve_triangular(factor_kk, jnp.eye(P_SIZE, dtype=matrix.dtype), lower=True)
            panel_rows = jnp.dot(matrix[finish:, begin_at:finish], inverse_kk.T, precision=lax.Precision.HIGHEST)
            update = jnp.dot(panel_rows, panel_rows.T, precision=lax.Precision.HIGHEST)
            matrix = matrix.at[finish:, finish:].add(-update)
            matrix = matrix.at[begin_at:finish, begin_at:finish].set(factor_kk)
            matrix = matrix.at[finish:, begin_at:finish].set(panel_rows)
            matrix = matrix.at[begin_at:finish, finish:].set(0.0)
        results.append(matrix[restore][:, restore])
    return jnp.stack(results)
```

```python
import jax
import jax.numpy as jnp
from jax import lax
from jax.experimental import pallas as pl
from jax.experimental.pallas import tpu as pltpu
from jax.sharding import PartitionSpec as P

P_SIZE = 512
STEPS = 2
BLK = 128
SUB = 8

damping_share = 0.03162277660168379
f32 = jnp.float32
bf16 = jnp.bfloat16


def split(x):
    hi = x.astype(bf16)
    return hi, (x - hi.astype(f32)).astype(bf16)


def dot3(a, b, dims=((1,), (0,))):
    (ah, al), (bh, bl) = a, b
    dn = (dims, ((), ()))
    out = lax.dot_general(ah, bh, dn, preferred_element_type=f32)
    out += lax.dot_general(ah, bl, dn, preferred_element_type=f32)
    return out + lax.dot_general(al, bh, dn, preferred_element_type=f32)


def factor_block(block, lane, sub):
    groups = BLK // SUB
    rows = [block[SUB * i : SUB * (i + 1), :] for i in range(groups)]
    upper, inverse = [], []
    row_of = lambda x, k: jnp.broadcast_to(x[k : k + 1, :], (SUB, BLK))
    col_of = lambda x, j: jnp.broadcast_to(x[:, j : j + 1], (SUB, BLK))
    for g in range(groups):
        first = SUB * g
        v = rows[g]
        cols = [col_of(v, first + k) for k in range(SUB)]
        raw = [[col_of(rows[i], first + k) for k in range(SUB)] for i in range(g + 1, groups)]
        va = jnp.where(lane >= first, v, 0.0)
        vb = jnp.where(lane < first, v, jnp.where(lane == sub + first, 1.0, 0.0))
        ra = jnp.zeros((SUB, BLK), f32)
        rb = jnp.zeros((SUB, BLK), f32)
        for k in range(SUB):
            pivot = row_of(cols[k], k)
            root = lax.rsqrt(pivot)
            recip = 1.0 / pivot
            here = sub == k
            ka, kb = row_of(va, k), row_of(vb, k)
            ra = jnp.where(here, ka * root, ra)
            rb = jnp.where(here, kb * root, rb)
            na, nb = ka * recip, kb * recip
            va = jnp.where(here, na, va - cols[k] * na)
            vb = jnp.where(here, nb, vb - cols[k] * nb)
            for m in range(k + 1, SUB):
                nm = row_of(cols[m], k) * recip
                cols[m] = jnp.where(here, nm, cols[m] - cols[k] * nm)
        upper.append(jnp.where(lane >= sub + first, ra, 0.0))
        inverse.append(jnp.where(lane <= sub + first, rb, 0.0))
        y = jnp.where(lane < first + SUB, vb, va)
        ys = [row_of(y, k) for k in range(SUB)]
        inside = (lane >= first) & (lane < first + SUB)
        for i in range(g + 1, groups):
            t = jnp.where(inside, 0.0, rows[i])
            for k in range(SUB):
                t = t - raw[i - g - 1][k] * ys[k]
            rows[i] = t
    return jnp.concatenate(upper, 0), jnp.concatenate(inverse, 0)


def factor_kernel(pieces, traces, lower, inv_hi, inv_lo, damp_out, w, diag_u, *, order, col_count, slab, assembled):
    n = STEPS * P_SIZE
    nb = n // BLK
    lane = lax.broadcasted_iota(jnp.int32, (SUB, BLK), 1)
    sub = lax.broadcasted_iota(jnp.int32, (SUB, BLK), 0)
    total = jnp.sum(traces[...]) * (1.0 / BLK)
    damp = damping_share * total / order
    damp_out[...] = jnp.full(damp_out.shape, damp, f32)
    if assembled:
        w[...] = pieces[...]
    else:
        for crow in range(col_count):
            for k in range(STEPS):
                top = k * P_SIZE + crow * slab
                per = pieces.shape[1] // (STEPS * slab)
                dev0 = crow // per * col_count
                begin = crow % per * STEPS * slab + k * slab
                for kk in range(STEPS):
                    parts = [
                        pieces[dev0 + c, begin : begin + slab, kk * slab : (kk + 1) * slab]
                        for c in range(col_count)
                    ]
                    w[top : top + slab, kk * P_SIZE : (kk + 1) * P_SIZE] = jnp.concatenate(parts, 1)
    eye = lax.broadcasted_iota(jnp.int32, (BLK, BLK), 0) == lax.broadcasted_iota(jnp.int32, (BLK, BLK), 1)
    for k in range(nb):
        at = slice(k * BLK, (k + 1) * BLK)
        w[at, at] = w[at, at] + jnp.where(eye, damp, 0.0)

    def step(k, _):
        here = pl.ds(pl.multiple_of(k * BLK, BLK), BLK)
        up, inv = factor_block(w[here, here], lane, sub)
        diag_u[here, :] = up
        w[here, :] = jnp.dot(inv, w[here, :], precision=lax.Precision.HIGHEST, preferred_element_type=f32)
        w[here, here] = inv

        def update(i, _):
            there = pl.ds(pl.multiple_of(i * BLK, BLK), BLK)
            left = w[here, there]
            w[there, here] = jnp.zeros((BLK, BLK), f32)
            w[there, :] = w[there, :] - lax.dot_general(
                left, w[here, :], (((0,), (0,)), ((), ())),
                precision=lax.Precision.HIGHEST, preferred_element_type=f32,
            )
            return 0

        lax.fori_loop(k + 1, nb, update, 0)
        return 0

    lax.fori_loop(0, nb, step, 0)
    for i in range(nb):
        ri = slice(i * BLK, (i + 1) * BLK)
        for j in range(nb):
            rj = slice(j * BLK, (j + 1) * BLK)
            if j <= i:
                lower[ri, rj] = (diag_u[ri, :] if i == j else w[rj, ri]).T
                hi, lo = split(w[ri, rj].T)
                inv_hi[rj, ri] = hi
                inv_lo[rj, ri] = lo
            else:
                lower[ri, rj] = jnp.zeros((BLK, BLK), f32)
                inv_hi[rj, ri] = jnp.zeros((BLK, BLK), bf16)
                inv_lo[rj, ri] = jnp.zeros((BLK, BLK), bf16)


def apply_kernel(
    coords, panel, cross, inv_hi, inv_lo, own_hi, own_lo, own_low, damp, work, out, cr, ch, cl, *, slab, cols_dev, rows_dev
):
    t = pl.program_id(0)
    tile = work.shape[0]
    col_count = panel.shape[0]
    width = STEPS * slab
    inverse = (inv_hi[...], inv_lo[...])

    @pl.when(t == 0)
    def _():
        for c in range(col_count):
            for k in range(STEPS):
                cr[k * P_SIZE + c * slab : k * P_SIZE + (c + 1) * slab, :] = cross[
                    c * width + k * slab : c * width + (k + 1) * slab, :
                ]
        hi, lo = split(dot3(inverse, split(cr[...]), ((0,), (0,))))
        ch[...] = hi
        cl[...] = lo

    rows = jnp.concatenate(
        [panel[c, :, k * slab : (k + 1) * slab] for k in range(STEPS) for c in range(col_count)], 1
    )
    rows = split(rows)
    left = split(dot3(rows, inverse))
    own = dot3(rows, (own_hi[...], own_lo[...]))
    update = dot3(left, (ch[...], cl[...]))
    row = lax.broadcasted_iota(jnp.int32, work.shape, 0) + (coords[0] * rows_dev + t * tile)
    col = lax.broadcasted_iota(jnp.int32, work.shape, 1) + coords[1] * cols_dev
    out[...] = work[...] + jnp.where(row == col, damp[0:1, 0:1], 0.0) - update
    out[:, 0:width] = own
    per = cols_dev // tile

    @pl.when(t % per == 0)
    def _():
        out[0:width, :] = jnp.zeros((width, cols_dev), f32)
        begin = pl.multiple_of(t // per * width, width)
        out[0:width, 0:width] = own_low[pl.ds(begin, width), :]


def on_device(factors):
    members, rows_dev, cols_dev = factors.shape
    col_count = lax.axis_size("col")
    row_count = lax.axis_size("row")
    order = rows_dev * row_count
    row_id = lax.axis_index("row")
    col_id = lax.axis_index("col")
    per_row = rows_dev // cols_dev
    slab = P_SIZE // col_count
    width = STEPS * slab
    n = STEPS * P_SIZE
    outs = []
    for member in range(members):
        local = factors[member]
        tall = local[:, :width]
        piece = jnp.concatenate([tall[b * cols_dev : b * cols_dev + width] for b in range(per_row)], 0)
        start = (col_id % per_row) * cols_dev
        on_diag = jnp.eye(BLK, dtype=f32) * (col_id // per_row == row_id)
        acc = jnp.zeros((BLK, BLK), f32)
        for b in range(cols_dev // BLK):
            acc += on_diag * lax.dynamic_slice(local, (start + b * BLK, b * BLK), (BLK, BLK))
        height = per_row * width
        assembled = slab % 64 != 0
        if assembled:
            traces = jnp.full((SUB, BLK), lax.psum(jnp.sum(acc), ("row", "col")) / SUB)
            pieces = lax.all_gather(piece, "col", axis=1, tiled=True)
            pieces = lax.all_gather(pieces, "row", axis=0, tiled=True)
            sequence = jnp.arange(n).reshape(col_count, STEPS, slab).transpose(1, 0, 2).reshape(n)
            pieces = jnp.take(jnp.take(pieces, sequence, axis=0).T, sequence, axis=0).T
        else:
            extra = jnp.broadcast_to(jnp.sum(acc), (SUB, width))
            pieces = lax.all_gather(jnp.concatenate([piece, extra], 0), ("row", "col"), axis=0)
            traces = jnp.broadcast_to(pieces[:, height, :1], (row_count * col_count, BLK))
        wide = jnp.concatenate([local[b * cols_dev : b * cols_dev + width] for b in range(per_row)], 0)
        panel = lax.all_gather(tall, "col", axis=0)
        cross = lax.all_gather(wide, "row", axis=0, tiled=True)

        def kernel(pieces, *rest):
            factor_kernel(
                pieces, *rest, order=order, col_count=col_count, slab=slab, assembled=assembled
            )

        if not assembled:
            def kernel(pieces, *rest, height=height):
                factor_kernel(
                    pieces.at[:, 0:height, :], *rest,
                    order=order, col_count=col_count, slab=slab, assembled=False,
                )

        lower, inv_hi, inv_lo, damp = pl.pallas_call(
            kernel,
            out_shape=(
                jax.ShapeDtypeStruct((n, n), f32),
                jax.ShapeDtypeStruct((n, n), bf16),
                jax.ShapeDtypeStruct((n, n), bf16),
                jax.ShapeDtypeStruct((SUB, BLK), f32),
            ),
            scratch_shapes=[pltpu.VMEM((n, n), f32), pltpu.VMEM((n, BLK), f32)],
            compiler_params=pltpu.CompilerParams(vmem_limit_bytes=60 * 1024 * 1024),
            cost_estimate=pl.CostEstimate(flops=40_000_000_000, bytes_accessed=12_000_000, transcendentals=0),
            name="factor",
        )(pieces, traces)
        split_cols = lambda x: lax.dynamic_slice_in_dim(
            x.reshape(x.shape[0], STEPS, col_count, slab), col_id, 1, 2
        ).reshape(x.shape[0], width)
        own_hi, own_lo = split_cols(inv_hi), split_cols(inv_lo)
        own_low = lax.dynamic_slice_in_dim(
            lower.reshape(STEPS, row_count, per_row, slab, n), row_id, 1, 1
        )
        own_low = split_cols(own_low[:, 0].transpose(1, 0, 2, 3).reshape(height, n))
        coords = jnp.stack([row_id, col_id]).astype(jnp.int32)
        tile = min(256, cols_dev)
        full = lambda a: pl.BlockSpec(a.shape, lambda t: (0,) * a.ndim)
        outs.append(pl.pallas_call(
            lambda *refs: apply_kernel(*refs, slab=slab, cols_dev=cols_dev, rows_dev=rows_dev),
            grid=(rows_dev // tile,),
            in_specs=[
                pl.BlockSpec(memory_space=pltpu.SMEM),
                pl.BlockSpec((col_count, tile, width), lambda t: (0, t, 0)),
                full(cross), full(inv_hi), full(inv_lo), full(own_hi), full(own_lo), full(own_low), full(damp),
                pl.BlockSpec((tile, cols_dev), lambda t: (t, 0)),
            ],
            out_specs=pl.BlockSpec((tile, cols_dev), lambda t: (t, 0)),
            out_shape=jax.ShapeDtypeStruct((rows_dev, cols_dev), f32),
            scratch_shapes=[
                pltpu.VMEM((n, cols_dev), f32),
                pltpu.VMEM((n, cols_dev), bf16),
                pltpu.VMEM((n, cols_dev), bf16),
            ],
            compiler_params=pltpu.CompilerParams(vmem_limit_bytes=60 * 1024 * 1024),
            name="apply",
        )(coords, panel, cross, inv_hi, inv_lo, own_hi, own_lo, own_low, damp, local))
    return jnp.stack(outs)


def solution(mesh):
    placed = (P(None, "row", "col"),)
    return jax.shard_map(
        on_device, mesh=mesh, in_specs=placed, out_specs=P(None, "row", "col"), check_vma=False
    )
```

```python
import jax
import jax.numpy as jnp
from jax import lax
from jax.experimental import pallas as pl
from jax.experimental.pallas import tpu as pltpu
from jax.sharding import PartitionSpec as P

P_SIZE = 512
STEPS = 2
BLK = 128
SUB = 8

damping_share = 0.03162277660168379
f32 = jnp.float32
bf16 = jnp.bfloat16


def split(x):
    hi = x.astype(bf16)
    return hi, (x - hi.astype(f32)).astype(bf16)


def dot3(a, b, dims=((1,), (0,))):
    (ah, al), (bh, bl) = a, b
    dn = (dims, ((), ()))
    out = lax.dot_general(ah, bh, dn, preferred_element_type=f32)
    out += lax.dot_general(ah, bl, dn, preferred_element_type=f32)
    return out + lax.dot_general(al, bh, dn, preferred_element_type=f32)


def factor_block(block, lane, sub):
    groups = BLK // SUB
    rows = [block[SUB * i : SUB * (i + 1), :] for i in range(groups)]
    upper, inverse = [], []
    row_of = lambda x, k: jnp.broadcast_to(x[k : k + 1, :], (SUB, BLK))
    col_of = lambda x, j: jnp.broadcast_to(x[:, j : j + 1], (SUB, BLK))
    for g in range(groups):
        first = SUB * g
        v = rows[g]
        cols = [col_of(v, first + k) for k in range(SUB)]
        raw = [[col_of(rows[i], first + k) for k in range(SUB)] for i in range(g + 1, groups)]
        va = jnp.where(lane >= first, v, 0.0)
        vb = jnp.where(lane < first, v, jnp.where(lane == sub + first, 1.0, 0.0))
        ra = jnp.zeros((SUB, BLK), f32)
        rb = jnp.zeros((SUB, BLK), f32)
        for k in range(SUB):
            pivot = row_of(cols[k], k)
            root = lax.rsqrt(pivot)
            recip = 1.0 / pivot
            here = sub == k
            ka, kb = row_of(va, k), row_of(vb, k)
            ra = jnp.where(here, ka * root, ra)
            rb = jnp.where(here, kb * root, rb)
            na, nb = ka * recip, kb * recip
            va = jnp.where(here, na, va - cols[k] * na)
            vb = jnp.where(here, nb, vb - cols[k] * nb)
            for m in range(k + 1, SUB):
                nm = row_of(cols[m], k) * recip
                cols[m] = jnp.where(here, nm, cols[m] - cols[k] * nm)
        upper.append(jnp.where(lane >= sub + first, ra, 0.0))
        inverse.append(jnp.where(lane <= sub + first, rb, 0.0))
        y = jnp.where(lane < first + SUB, vb, va)
        ys = [row_of(y, k) for k in range(SUB)]
        inside = (lane >= first) & (lane < first + SUB)
        for i in range(g + 1, groups):
            t = jnp.where(inside, 0.0, rows[i])
            for k in range(SUB):
                t = t - raw[i - g - 1][k] * ys[k]
            rows[i] = t
    return jnp.concatenate(upper, 0), jnp.concatenate(inverse, 0)


def factor_kernel(
    pieces, traces, lower, inv_hi, inv_lo, damp_out, w, diag_u, turned, stack_l, stack_r, *, order, col_count, slab, assembled
):
    n = STEPS * P_SIZE
    nb = n // BLK
    lane = lax.broadcasted_iota(jnp.int32, (SUB, BLK), 1)
    sub = lax.broadcasted_iota(jnp.int32, (SUB, BLK), 0)
    total = jnp.sum(traces[...]) * (1.0 / BLK)
    damp = damping_share * total / order
    damp_out[...] = jnp.full(damp_out.shape, damp, f32)
    if assembled:
        w[...] = pieces[...]
    else:
        for crow in range(col_count):
            for k in range(STEPS):
                top = k * P_SIZE + crow * slab
                per = pieces.shape[1] // (STEPS * slab)
                dev0 = crow // per * col_count
                begin = crow % per * STEPS * slab + k * slab
                for kk in range(STEPS):
                    parts = [
                        pieces[dev0 + c, begin : begin + slab, kk * slab : (kk + 1) * slab]
                        for c in range(col_count)
                    ]
                    w[top : top + slab, kk * P_SIZE : (kk + 1) * P_SIZE] = jnp.concatenate(parts, 1)
    eye = lax.broadcasted_iota(jnp.int32, (BLK, BLK), 0) == lax.broadcasted_iota(jnp.int32, (BLK, BLK), 1)
    for k in range(nb):
        at = slice(k * BLK, (k + 1) * BLK)
        w[at, at] = w[at, at] + jnp.where(eye, damp, 0.0)

    def step(k, _):
        here = pl.ds(pl.multiple_of(k * BLK, BLK), BLK)
        up, inv = factor_block(w[here, here], lane, sub)
        diag_u[here, :] = up
        w[here, :] = jnp.dot(inv, w[here, :], precision=lax.Precision.HIGHEST, preferred_element_type=f32)
        w[here, here] = inv
        hi, lo = split(w[here, :])
        for part, (x, y) in enumerate(((hi, hi), (hi, lo), (lo, hi))):
            stack_l[part * BLK : (part + 1) * BLK, :] = x
            stack_r[part * BLK : (part + 1) * BLK, :] = y

        def update(i, _):
            there = pl.ds(pl.multiple_of(i * BLK, BLK), BLK)
            w[there, here] = jnp.zeros((BLK, BLK), f32)
            w[there, :] = w[there, :] - lax.dot_general(
                stack_l[:, there], stack_r[...], (((0,), (0,)), ((), ())), preferred_element_type=f32
            )
            return 0

        lax.fori_loop(k + 1, nb, update, 0)
        return 0

    lax.fori_loop(0, nb, step, 0)

    def strips(store):
        if assembled:
            store(slice(0, n), turned[...])
            return
        for c in range(col_count):
            for k in range(STEPS):
                top = k * P_SIZE + c * slab
                line = turned[top : top + slab, :]
                parts = [
                    line[:, kk * P_SIZE + cc * slab : kk * P_SIZE + (cc + 1) * slab]
                    for cc in range(col_count)
                    for kk in range(STEPS)
                ]
                first = (c * STEPS + k) * slab
                store(slice(first, first + slab), jnp.concatenate(parts, 1))

    def store_lower(at, x):
        lower[at, :] = x

    def store_inverse(at, x):
        inv_hi[at, :], inv_lo[at, :] = split(x)

    at = lambda i: slice(i * BLK, (i + 1) * BLK)
    turned[...] = jnp.zeros(turned.shape, f32)
    for i in range(nb):
        for j in range(i + 1):
            turned[at(i), at(j)] = (diag_u[at(i), :] if i == j else w[at(j), at(i)]).T
    strips(store_lower)
    turned[...] = jnp.zeros(turned.shape, f32)
    for i in range(nb):
        for j in range(i + 1):
            turned[at(j), at(i)] = w[at(i), at(j)].T
    strips(store_inverse)


def apply_kernel(
    coords, panel, inv_hi, inv_lo, own_hi, own_lo, own_low, damp, work, *rest, slab, cols_dev, rows_dev
):
    *cross, out, cr, ch, cl = rest
    t = pl.program_id(0)
    tile = work.shape[0]
    col_count = panel.shape[0]
    width = STEPS * slab
    inverse = (inv_hi[...], inv_lo[...])

    @pl.when(t == 0)
    def _():
        for shift, piece in enumerate(cross):
            height = piece.shape[0]
            begin = pl.multiple_of((coords[0] + shift) % len(cross) * height, height)
            cr[pl.ds(begin, height), :] = piece[...]
        hi, lo = split(dot3(inverse, split(cr[...]), ((0,), (0,))))
        ch[...] = hi
        cl[...] = lo

    rows = jnp.concatenate([panel[c] for c in range(col_count)], 1)
    rows = split(rows)
    left = split(dot3(rows, inverse))
    own = dot3(rows, (own_hi[...], own_lo[...]))
    update = dot3(left, (ch[...], cl[...]))
    row = lax.broadcasted_iota(jnp.int32, work.shape, 0) + (coords[0] * rows_dev + t * tile)
    col = lax.broadcasted_iota(jnp.int32, work.shape, 1) + coords[1] * cols_dev
    out[...] = work[...] + jnp.where(row == col, damp[0:1, 0:1], 0.0) - update
    out[:, 0:width] = own
    per = cols_dev // tile

    @pl.when(t % per == 0)
    def _():
        out[0:width, :] = jnp.zeros((width, cols_dev), f32)
        begin = pl.multiple_of(t // per * width, width)
        out[0:width, 0:width] = own_low[pl.ds(begin, width), :]


def on_device(factors):
    members, rows_dev, cols_dev = factors.shape
    col_count = lax.axis_size("col")
    row_count = lax.axis_size("row")
    order = rows_dev * row_count
    row_id = lax.axis_index("row")
    col_id = lax.axis_index("col")
    per_row = rows_dev // cols_dev
    slab = P_SIZE // col_count
    width = STEPS * slab
    n = STEPS * P_SIZE
    outs = []
    for member in range(members):
        local = factors[member]
        tall = local[:, :width]
        piece = jnp.concatenate([tall[b * cols_dev : b * cols_dev + width] for b in range(per_row)], 0)
        start = (col_id % per_row) * cols_dev
        on_diag = jnp.eye(BLK, dtype=f32) * (col_id // per_row == row_id)
        acc = jnp.zeros((BLK, BLK), f32)
        for b in range(cols_dev // BLK):
            acc += on_diag * lax.dynamic_slice(local, (start + b * BLK, b * BLK), (BLK, BLK))
        height = per_row * width
        assembled = slab % 64 != 0
        if assembled:
            traces = jnp.full((SUB, BLK), lax.psum(jnp.sum(acc), ("row", "col")) / SUB)
            pieces = lax.all_gather(piece, "col", axis=1, tiled=True)
            pieces = lax.all_gather(pieces, "row", axis=0, tiled=True)
            sequence = jnp.arange(n).reshape(col_count, STEPS, slab).transpose(1, 0, 2).reshape(n)
            pieces = jnp.take(jnp.take(pieces, sequence, axis=0).T, sequence, axis=0).T
        else:
            extra = jnp.broadcast_to(jnp.sum(acc), (SUB, width))
            pieces = lax.all_gather(jnp.concatenate([piece, extra], 0), ("row", "col"), axis=0)
            traces = jnp.broadcast_to(pieces[:, height, :1], (row_count * col_count, BLK))
        wide = jnp.concatenate([local[b * cols_dev : b * cols_dev + width] for b in range(per_row)], 0)
        panel = lax.all_gather(tall, "col", axis=0)
        shifted = [
            lax.ppermute(wide, "row", [(i, (i - shift) % row_count) for i in range(row_count)])
            for shift in range(1, row_count)
        ]
        cross = [wide] + shifted

        def kernel(pieces, *rest):
            factor_kernel(
                pieces, *rest, order=order, col_count=col_count, slab=slab, assembled=assembled
            )

        if not assembled:
            def kernel(pieces, *rest, height=height):
                factor_kernel(
                    pieces.at[:, 0:height, :], *rest,
                    order=order, col_count=col_count, slab=slab, assembled=False,
                )

        lower, inv_hi, inv_lo, damp = pl.pallas_call(
            kernel,
            out_shape=(
                jax.ShapeDtypeStruct((n, n), f32),
                jax.ShapeDtypeStruct((n, n), bf16),
                jax.ShapeDtypeStruct((n, n), bf16),
                jax.ShapeDtypeStruct((SUB, BLK), f32),
            ),
            scratch_shapes=[
                pltpu.VMEM((n, n), f32),
                pltpu.VMEM((n, BLK), f32),
                pltpu.VMEM((n, n), f32),
                pltpu.VMEM((3 * BLK, n), bf16),
                pltpu.VMEM((3 * BLK, n), bf16),
            ],
            compiler_params=pltpu.CompilerParams(vmem_limit_bytes=60 * 1024 * 1024),
            cost_estimate=pl.CostEstimate(flops=40_000_000_000, bytes_accessed=12_000_000, transcendentals=0),
            name="factor",
        )(pieces, traces)
        if assembled:
            sequence = jnp.arange(n).reshape(STEPS, col_count, slab).transpose(1, 0, 2).reshape(n)
            reorder = lambda x: jnp.take(jnp.take(x, sequence, axis=0).T, sequence, axis=0).T
            lower, inv_hi, inv_lo = reorder(lower), reorder(inv_hi), reorder(inv_lo)
            own = lambda x: lax.dynamic_slice_in_dim(x, col_id * width, width, 1)
            own_hi, own_lo = own(inv_hi), own(inv_lo)
            own_low = own(lax.dynamic_slice_in_dim(lower, row_id * height, height, 0))
            own_row = own_col = lambda t, at: (0, 0)
        else:
            own_hi, own_lo, own_low = inv_hi, inv_lo, lower
            own_col = lambda t, at: (0, at[1])
            own_row = lambda t, at: (at[0], at[1])
        coords = jnp.stack([row_id, col_id]).astype(jnp.int32)
        tile = min(256, cols_dev)
        full = lambda a: pl.BlockSpec(a.shape, lambda t, at: (0,) * a.ndim)
        outs.append(pl.pallas_call(
            lambda *refs: apply_kernel(*refs, slab=slab, cols_dev=cols_dev, rows_dev=rows_dev),
            grid_spec=pltpu.PrefetchScalarGridSpec(
                num_scalar_prefetch=1,
                grid=(rows_dev // tile,),
                in_specs=[
                    pl.BlockSpec((col_count, tile, width), lambda t, at: (0, t, 0)),
                    full(inv_hi), full(inv_lo),
                    pl.BlockSpec((n, width), own_col),
                    pl.BlockSpec((n, width), own_col),
                    pl.BlockSpec((height, width), own_row),
                    full(damp),
                    pl.BlockSpec((tile, cols_dev), lambda t, at: (t, 0)),
                    *[full(x) for x in cross],
                ],
                out_specs=pl.BlockSpec((tile, cols_dev), lambda t, at: (t, 0)),
                scratch_shapes=[
                    pltpu.VMEM((n, cols_dev), f32),
                    pltpu.VMEM((n, cols_dev), bf16),
                    pltpu.VMEM((n, cols_dev), bf16),
                ],
            ),
            out_shape=jax.ShapeDtypeStruct((rows_dev, cols_dev), f32),
            compiler_params=pltpu.CompilerParams(vmem_limit_bytes=60 * 1024 * 1024),
            name="apply",
        )(coords, panel, inv_hi, inv_lo, own_hi, own_lo, own_low, damp, local, *cross))
    return jnp.stack(outs)


def solution(mesh):
    placed = (P(None, "row", "col"),)
    return jax.shard_map(
        on_device, mesh=mesh, in_specs=placed, out_specs=P(None, "row", "col"), check_vma=False
    )
```
